128 devices in a mesh: tm: 32 (over z, y, core), freq: 4 (over x).
Axes of the slice: x: 4, y: 4, z: 4, core: 2. Of those that a mesh axis runs over, the one named last changes fastest.
Arguments:
- spectrum: bfloat16 [4096, 262144], P('freq', 'tm'), may hold values from 4 to 160
- templates: float32 [4096, 128], P('freq'), may hold values from 0.02 to 2.1
- activations: float32 [128, 262144], P(None, 'tm'), may hold values from 0.06 to 6
- lengths: int32 [512], P('tm'), may hold values from 1 to 512
Outputs:
- new_activations: float32 [128, 262144], P(None, 'tm')
- new_templates: float32 [4096, 128], P('freq')
The draws below stay inside these ranges and needn't reach their ends.
Inputs may be any that keep to these rules, and one draw needn't show every extreme that they name: Track j holds frame slots j * 512 to (j + 1) * 512 - 1; its first lengths[j] slots are frames, the rest padding whose spectrum is arbitrary.
All inputs are finite; a program needn't handle non-finite values.
Results may differ from the reference program's by a relative error of at most 0.0003.
Values sent between devices are 32-bit elements; how exact they have to be, the bound alone decides.
A program may use at most 128 MiB of HBM per device.

```python
import math
import jax
import jax.numpy as jnp
from jax import lax

F = 4096
K = 128
TRACK_LEN = 512
UPDATES = 2
FRAMES = 262144
TRACKS = 512


def band_table(table_key, rows, count):
    center_key, width_key, rough_key = jax.random.split(table_key, 3)
    band_centers = jax.random.uniform(center_key, (1, count), jnp.float32, 0.0, rows * 1.0)
    band_widths = jnp.exp(jax.random.uniform(width_key, (1, count), jnp.float32, math.log(rows / 64.0), math.log(rows / 8.0)))
    bin_index = lax.broadcasted_iota(jnp.float32, (rows, count), 0)
    offset_ratio = (bin_index - band_centers) / band_widths
    profile = jnp.exp(-0.5 * offset_ratio * offset_ratio)
    roughness = jnp.exp(jax.random.uniform(rough_key, (rows, count), jnp.float32, math.log(0.5), math.log(2.0)))
    return profile * roughness


def draw_spectrum(key, part):
    table_key, choose_key, gain_key, jitter_key = jax.random.split(jax.random.fold_in(key, 11), 4)
    profiles = band_table(table_key, F, K)
    component_ids = jax.random.randint(choose_key, (TRACKS, TRACK_LEN, 3), 0, K)
    gain_values = jnp.exp(jax.random.uniform(gain_key, (TRACKS, TRACK_LEN, 3), jnp.float32, math.log(5.0), math.log(70.0)))

    def one_block(block_index):
        block_ids = component_ids[block_index]
        block_gains = gain_values[block_index]
        summed = jnp.full((F, TRACK_LEN), 4.0, jnp.float32)
        for slot_index in range(3):
            summed = summed + jnp.take(profiles, block_ids[:, slot_index], axis=1) * block_gains[None, :, slot_index]
        block_key = jax.random.fold_in(jitter_key, block_index)
        jitter_factor = jnp.exp(jax.random.uniform(block_key, (F, TRACK_LEN), jnp.float32, math.log(0.6), math.log(1.6)))
        return jnp.clip(summed * jitter_factor, 4.0, 160.0).astype(jnp.bfloat16)
    blocks = lax.map(one_block, jnp.arange(TRACKS, dtype=jnp.int32))
    return jnp.transpose(blocks, (1, 0, 2)).reshape(F, FRAMES)


def draw_templates(key, part):
    table_key, base_key = jax.random.split(jax.random.fold_in(key, 23), 2)
    profiles = band_table(table_key, F, K)
    base_level = jax.random.uniform(base_key, (F, K), jnp.float32, 0.02, 0.1)
    return base_level + profiles


def draw_activations(key, part):
    scale_key, entry_key = jax.random.split(jax.random.fold_in(key, 37), 2)
    frame_scale = jnp.exp(jax.random.uniform(scale_key, (1, FRAMES), jnp.float32, math.log(0.3), math.log(3.0)))
    entries = jnp.exp(jax.random.uniform(entry_key, (K, FRAMES), jnp.float32, math.log(0.2), math.log(2.0)))
    return frame_scale * entries


def plant(values, rng, least, largest):
    longest = values.shape.index(max(values.shape))
    spots = []
    for shift in (0, 1):
        where = [jax.random.randint(jax.random.fold_in(rng, axis), (), 0, length) for axis, length in enumerate(values.shape)]
        where[longest] = (where[longest] + shift) % values.shape[longest]
        spots.append(tuple(where))
    return values.at[spots[0]].set(least).at[spots[1]].set(largest)


def setup_inputs(seed: int = 0) -> dict:
    key_of = jax.random.split(jax.random.key(seed), 5)
    return {
        "spectrum": draw_spectrum(jax.random.fold_in(key_of[4], 71), 0),
        "templates": draw_templates(jax.random.fold_in(key_of[4], 71), 0),
        "activations": draw_activations(jax.random.fold_in(key_of[4], 71), 0),
        "lengths": plant(jax.random.randint(key_of[3], (TRACKS,), 1, TRACK_LEN + 1), jax.random.fold_in(key_of[3], 1), 1, TRACK_LEN).astype(jnp.int32),
    }


def alive_frames(lengths):
    position = lax.broadcasted_iota(jnp.int32, (lengths.shape[0], TRACK_LEN), 1)
    return (position < lengths[:, None]).reshape(-1)


def refine(current, numerator, weight_gram, alive_mask):
    for repeat_index in range(UPDATES):
        denominator = jnp.dot(weight_gram, current, precision=lax.Precision.HIGHEST)
        denominator = jnp.where(alive_mask[None, :], denominator, 1.0)
        current = jnp.where(alive_mask[None, :], current * numerator / denominator, 0.0)
    return current


def reference(spectrum, templates, activations, lengths):
    alive_mask = alive_frames(lengths)
    low_templates = templates.astype(jnp.bfloat16)
    numerator = jnp.dot(low_templates.T, spectrum, preferred_element_type=jnp.float32)
    weight_gram = jnp.dot(templates.T, templates, precision=lax.Precision.HIGHEST)
    current = refine(activations, numerator, weight_gram, alive_mask)
    low_activations = current.astype(jnp.bfloat16)
    cross = jnp.dot(spectrum, low_activations.T, preferred_element_type=jnp.float32)
    frame_gram = jnp.dot(current, current.T, precision=lax.Precision.HIGHEST)
    updated = templates * cross / jnp.dot(templates, frame_gram, precision=lax.Precision.HIGHEST)
    return current, updated
```

```python
import functools

import jax
import jax.numpy as jnp
from jax import lax
from jax.experimental import pallas as pl
from jax.experimental.pallas import tpu as pltpu
from jax.sharding import PartitionSpec as P

MESH = pl.DeviceIdType.MESH
TRACK_LEN = 512
UPDATES = 2
CHUNKS = 8
SIZES = (2048, 4096, 4608, 5120, 5632, 6144, 7168, 8192)
VMEM_LIMIT = 48 * 1024 * 1024

F32 = jnp.float32
BF16 = jnp.bfloat16
VMEM = pltpu.VMEM


def split(x):
    high = x.astype(BF16)
    low = (x - high.astype(F32)).astype(BF16)
    return high, low


def right_operand(m):
    high, low = split(m)
    top = jnp.concatenate([high, low], axis=1)
    bottom = jnp.concatenate([high, jnp.zeros_like(low)], axis=1)
    return jnp.concatenate([top, bottom], axis=0)


def fine_dot(x, operand):
    high, low = split(x)
    both = jnp.dot(jnp.concatenate([high, low], axis=1), operand, preferred_element_type=F32)
    k = both.shape[1] // 2
    return both[:, :k] + both[:, k:]


def fold_quadrants(m):
    k = m.shape[0] // 2
    return (m[:k, :k] + m[k:, k:]) + (m[:k, k:] + m[k:, :k])


def send(src, dst, send_sem, recv_sem, device):
    return pltpu.make_async_remote_copy(
        src_ref=src, dst_ref=dst, send_sem=send_sem, recv_sem=recv_sem,
        device_id=device, device_id_type=MESH,
    )


def numerator_kernel(
    ntm, nfreq, steps, spec_ref, templates_ref, act_ref, count_ref,
    num_ref, act_out_ref, operand_ref, most_ref,
    low_ref, gram_ref, grams_ref, counts_ref, gram_send, gram_recv, count_send, count_recv,
):
    step = pl.program_id(0)
    t = lax.axis_index("tm")
    r = lax.axis_index("freq")

    @pl.when(step == 0)
    def _():
        barrier = pltpu.get_barrier_semaphore()

        @pl.loop(1, ntm)
        def _(k):
            pl.semaphore_signal(barrier, inc=1, device_id=(lax.rem(t + k, ntm), r), device_id_type=MESH)

        @pl.loop(1, nfreq)
        def _(k):
            pl.semaphore_signal(barrier, inc=1, device_id=(t, lax.rem(r + k, nfreq)), device_id_type=MESH)

        turned = templates_ref[...].T
        high_t, low_t = split(turned)
        low_ref[...] = high_t
        high, low = split(templates_ref[...])
        products = jnp.dot(
            jnp.concatenate([high_t, low_t], axis=0),
            jnp.concatenate([high, low], axis=1),
            preferred_element_type=F32,
        )
        gram_ref[...] = fold_quadrants(products)
        pl.semaphore_wait(barrier, ntm + nfreq - 2)

        @pl.loop(1, ntm)
        def _(k):
            send(count_ref, counts_ref.at[k - 1], count_send, count_recv, (lax.rem(t + k, ntm), r)).start()

        for k in range(1, nfreq):
            send(gram_ref, grams_ref.at[k - 1], gram_send.at[k - 1], gram_recv.at[k - 1], (t, lax.rem(r + k, nfreq))).start()

    num = jnp.dot(low_ref[...], spec_ref[...], preferred_element_type=F32)
    num_ref[...] = num.T.reshape(num_ref.shape)
    act_out_ref[...] = act_ref[...].T.reshape(act_out_ref.shape)

    @pl.when(step == steps - 1)
    def _():
        everyone = send(counts_ref, counts_ref, count_send, count_recv, (lax.rem(t + 1, ntm), r))
        everyone.wait_send()
        everyone.wait_recv()
        most = count_ref[...]
        for k in range(ntm - 1):
            most = jnp.maximum(most, counts_ref[k])
        most_ref[...] = most
        gram = gram_ref[...]
        for k in range(1, nfreq):
            copy = send(gram_ref, grams_ref.at[k - 1], gram_send.at[k - 1], gram_recv.at[k - 1], (t, lax.rem(r + k, nfreq)))
            copy.wait_send()
            copy.wait_recv()
            gram = gram + grams_ref[k - 1]
        operand_ref[...] = right_operand(gram)


def numerator_call(mesh, spectrum, templates, activations, count):
    ntm, nfreq = mesh.shape["tm"], mesh.shape["freq"]
    bins, frames = spectrum.shape
    k = templates.shape[1]
    steps = frames // TRACK_LEN
    whole = lambda *shape: pl.BlockSpec(shape, lambda i: (0,) * len(shape))
    return pl.pallas_call(
        functools.partial(numerator_kernel, ntm, nfreq, steps),
        grid=(steps,),
        out_shape=(
            jax.ShapeDtypeStruct((frames // 8, 8, k), F32),
            jax.ShapeDtypeStruct((frames // 8, 8, k), F32),
            jax.ShapeDtypeStruct((2 * k, 2 * k), BF16),
            jax.ShapeDtypeStruct((8, 128), F32),
        ),
        in_specs=[
            pl.BlockSpec((bins, TRACK_LEN), lambda i: (0, i)),
            whole(bins, k),
            pl.BlockSpec((k, TRACK_LEN), lambda i: (0, i)),
            whole(8, 128),
        ],
        out_specs=(
            pl.BlockSpec((TRACK_LEN // 8, 8, k), lambda i: (i, 0, 0)),
            pl.BlockSpec((TRACK_LEN // 8, 8, k), lambda i: (i, 0, 0)),
            whole(2 * k, 2 * k),
            whole(8, 128),
        ),
        scratch_shapes=[
            VMEM((k, bins), BF16),
            VMEM((k, k), F32),
            VMEM((nfreq - 1, k, k), F32),
            VMEM((ntm - 1, 8, 128), F32),
            pltpu.SemaphoreType.DMA((nfreq - 1,)),
            pltpu.SemaphoreType.DMA((nfreq - 1,)),
            pltpu.SemaphoreType.DMA,
            pltpu.SemaphoreType.DMA,
        ],
        compiler_params=pltpu.CompilerParams(
            collective_id=0, has_side_effects=True, vmem_limit_bytes=VMEM_LIMIT,
            dimension_semantics=("arbitrary",),
        ),
        name="numerator",
    )(spectrum, templates, activations, count)


def refine_kernel(
    size, src_ref, num_ref, act_ref, operand_ref, out_ref,
    comp, own, first, direct, second, send_sem, first_sem, direct_sem, second_sem, near_sem, far_sem,
):
    t = lax.axis_index("tm")
    r = lax.axis_index("freq")
    shard, half = size // 4, size // 8
    cw = half // CHUNKS
    right, left, opposite = lax.rem(r + 1, 4), lax.rem(r + 3, 4), lax.rem(r + 2, 4)
    near = ((t, right), (t, left))

    barrier = pltpu.get_barrier_semaphore()
    for device in near:
        pl.semaphore_signal(barrier, inc=1, device_id=device, device_id_type=MESH)

    def rows(base, h, c):
        return pl.ds(pl.multiple_of(base * shard + h * half + c * cw, 8), cw)

    def part(c):
        return pl.ds(pl.multiple_of(c * cw, 8), cw)

    def gather(base, h, c, table, into, offset):
        start = base * shard + h * half + c * cw
        for i in range(cw // 8):
            source = src_ref[start // 8 + i]
            into[pl.ds(pl.multiple_of(start - offset + 8 * i, 8), 8), :] = table[source]

    def first_copy(way, c):
        return send(comp.at[rows(opposite, way, c)], first.at[way, part(c)], send_sem.at[way], first_sem.at[way, c], near[way])

    def direct_copy(way, c):
        return send(comp.at[rows((right, left)[way], 1 - way, c)], direct.at[way, part(c)], send_sem.at[2 + way], direct_sem.at[way, c], near[way])

    def second_copy(way, c):
        return send(first.at[way, part(c)], second.at[way, part(c)], send_sem.at[4 + way], second_sem.at[way, c], near[way])

    def near_copy(way, h, c):
        return send(out_ref.at[rows(r, h, c)], out_ref.at[rows(r, h, c)], send_sem.at[6 + 2 * way + h], near_sem.at[way, h, c], near[way])

    def near_arrival(way, h, c):
        owner = (left, right)[way]
        return send(out_ref.at[rows(owner, h, c)], out_ref.at[rows(owner, h, c)], send_sem.at[6 + 2 * way + h], near_sem.at[way, h, c], near[way])

    def far_copy(way, c):
        owner = (left, right)[way]
        return send(out_ref.at[rows(owner, way, c)], out_ref.at[rows(owner, way, c)], send_sem.at[10 + way], far_sem.at[way, c], near[way])

    def far_arrival(way, c):
        return send(out_ref.at[rows(opposite, way, c)], out_ref.at[rows(opposite, way, c)], send_sem.at[10 + way], far_sem.at[way, c], near[way])

    for way in range(2):
        gather(opposite, way, 0, num_ref, comp, 0)
    pl.semaphore_wait(barrier, 2)
    for way in range(2):
        first_copy(way, 0).start()

    @pl.loop(1, CHUNKS)
    def _(c):
        for way in range(2):
            gather(opposite, way, c, num_ref, comp, 0)
            first_copy(way, c).start()

    @pl.loop(0, CHUNKS)
    def _(c):
        for way in range(2):
            gather((right, left)[way], 1 - way, c, num_ref, comp, 0)
            direct_copy(way, c).start()

    @pl.loop(0, CHUNKS)
    def _(c):
        for way in range(2):
            gather((right, left)[way], way, c, num_ref, comp, 0)
            gather(r, way, c, num_ref, comp, 0)
            gather(r, way, c, act_ref, own, r * shard)

    @pl.loop(0, CHUNKS)
    def _(c):
        for way in range(2):
            first_copy(way, c).wait_recv()
            first[way, part(c), :] = first[way, part(c), :] + comp[rows((right, left)[way], way, c), :]
            second_copy(way, c).start()

    @pl.loop(0, CHUNKS)
    def _(c):
        for h in range(2):
            second_copy(h, c).wait_recv()
            direct_copy(1 - h, c).wait_recv()
            numerator = comp[rows(r, h, c), :] + second[h, part(c), :] + direct[1 - h, part(c), :]
            current = own[pl.ds(pl.multiple_of(h * half + c * cw, 8), cw), :]
            for _ in range(UPDATES):
                current = current * numerator / fine_dot(current, operand_ref[...])
            out_ref[rows(r, h, c), :] = current
            for way in range(2):
                near_copy(way, h, c).start()

    @pl.loop(0, CHUNKS)
    def _(c):
        for way in range(2):
            near_arrival(way, way, c).wait_recv()
            far_copy(way, c).start()

    @pl.loop(0, CHUNKS)
    def _(c):
        for way in range(2):
            near_arrival(way, 1 - way, c).wait_recv()
            far_arrival(way, c).wait_recv()

    for i in range(12):
        whole = first.at[0]
        send(whole, whole, send_sem.at[i], first_sem.at[0, 0], near[0]).wait_send()


def refine_call(size, index, src, num, act, operand):
    frames, k = num.shape[0] * 8, num.shape[2]
    shard, half = size // 4, size // 8
    whole = pl.BlockSpec(memory_space=VMEM)
    return pl.pallas_call(
        functools.partial(refine_kernel, size),
        out_shape=jax.ShapeDtypeStruct((frames, k), F32),
        in_specs=[pl.BlockSpec(memory_space=pltpu.SMEM), whole, whole, whole],
        out_specs=whole,
        scratch_shapes=[
            VMEM((size, k), F32),
            VMEM((shard, k), F32),
            VMEM((2, half, k), F32),
            VMEM((2, half, k), F32),
            VMEM((2, half, k), F32),
            pltpu.SemaphoreType.DMA((12,)),
            pltpu.SemaphoreType.DMA((2, CHUNKS)),
            pltpu.SemaphoreType.DMA((2, CHUNKS)),
            pltpu.SemaphoreType.DMA((2, CHUNKS)),
            pltpu.SemaphoreType.DMA((2, 2, CHUNKS)),
            pltpu.SemaphoreType.DMA((2, CHUNKS)),
        ],
        compiler_params=pltpu.CompilerParams(
            collective_id=2 + index, has_side_effects=True, vmem_limit_bytes=VMEM_LIMIT,
        ),
        name=f"refine_{size}",
    )(src, num, act, operand)


def cross_kernel(steps, start_ref, length_ref, act_ref, spec_ref, templates_ref, out_ref, cross_ref, denominator_ref, gram_ref):
    step = pl.program_id(0)
    x = act_ref[pl.ds(pl.multiple_of(start_ref[step], 8), TRACK_LEN), :]
    position = lax.broadcasted_iota(jnp.int32, x.shape, 0)
    x = jnp.where(position < length_ref[step], x, 0.0)
    turned = x.T
    out_ref[...] = turned
    high, low = split(x)
    high_t, low_t = split(turned)
    products = jnp.dot(
        jnp.concatenate([high_t, low_t], axis=0),
        jnp.concatenate([high, low], axis=1),
        preferred_element_type=F32,
    )
    cross = jnp.dot(spec_ref[...], high, preferred_element_type=F32)

    @pl.when(step == 0)
    def _():
        gram_ref[...] = products
        cross_ref[...] = cross

    @pl.when(step > 0)
    def _():
        gram_ref[...] += products
        cross_ref[...] += cross

    @pl.when(step == steps - 1)
    def _():
        denominator_ref[...] = fine_dot(templates_ref[...], right_operand(fold_quadrants(gram_ref[...])))


def cross_call(starts, lengths, act, spectrum, templates):
    bins, frames = spectrum.shape
    k = templates.shape[1]
    steps = frames // TRACK_LEN
    whole = lambda *shape: pl.BlockSpec(shape, lambda i, *_: (0,) * len(shape))
    return pl.pallas_call(
        functools.partial(cross_kernel, steps),
        grid_spec=pltpu.PrefetchScalarGridSpec(
            num_scalar_prefetch=2,
            grid=(steps,),
            in_specs=[
                whole(frames, k),
                pl.BlockSpec((bins, TRACK_LEN), lambda i, *_: (0, i)),
                whole(bins, k),
            ],
            out_specs=(
                pl.BlockSpec((k, TRACK_LEN), lambda i, *_: (0, i)),
                whole(bins, k),
                whole(bins, k),
            ),
            scratch_shapes=[VMEM((2 * k, 2 * k), F32)],
        ),
        out_shape=(
            jax.ShapeDtypeStruct((k, frames), F32),
            jax.ShapeDtypeStruct((bins, k), F32),
            jax.ShapeDtypeStruct((bins, k), F32),
        ),
        compiler_params=pltpu.CompilerParams(vmem_limit_bytes=VMEM_LIMIT, dimension_semantics=("arbitrary",)),
        name="cross",
    )(starts, lengths, act, spectrum, templates)


def template_kernel(
    ntm, cross_ref, denominator_ref, templates_ref, out_ref,
    pair, acc, land, pair_send, pair_recv, land_send, land_recv, out_send, out_recv, last_send, last_recv,
):
    t = lax.axis_index("tm")
    r = lax.axis_index("freq")
    places = ntm // 2
    core = lax.rem(t, 2)
    place = t // 2
    partner = (place * 2 + 1 - core, r)
    half = cross_ref.shape[0] // 2
    count = half // places

    def peer(k):
        return lax.rem(place + k, places)

    barrier = pltpu.get_barrier_semaphore()
    pl.semaphore_signal(barrier, inc=1, device_id=partner, device_id_type=MESH)

    @pl.loop(1, places)
    def _(k):
        pl.semaphore_signal(barrier, inc=1, device_id=(peer(k) * 2 + core, r), device_id_type=MESH)

    pl.semaphore_wait(barrier, places)

    mine = pl.ds(pl.multiple_of(core * half, 8), half)
    theirs = pl.ds(pl.multiple_of((1 - core) * half, 8), half)
    copies = [
        send(ref.at[theirs], pair.at[i], pair_send.at[i], pair_recv.at[i], partner)
        for i, ref in enumerate((cross_ref, denominator_ref))
    ]
    for copy in copies:
        copy.start()
    for i, (copy, ref) in enumerate(zip(copies, (cross_ref, denominator_ref))):
        copy.wait_recv()
        acc[i] = ref[mine, :] + pair[i]

    def piece(k):
        rows = pl.ds(pl.multiple_of(peer(k) * count, 8), count)
        return send(acc.at[:, rows], land.at[k - 1], land_send, land_recv, (peer(k) * 2 + core, r))

    @pl.loop(1, places)
    def _(k):
        piece(k).start()

    arrivals = send(land, land, land_send, land_recv, partner)
    arrivals.wait_recv()
    rows = pl.ds(pl.multiple_of(place * count, 8), count)
    total = acc[:, rows, :]
    for k in range(1, places):
        total = total + land[k - 1]
    own = pl.ds(pl.multiple_of(core * half + place * count, 8), count)
    out_ref[own, :] = templates_ref[own, :] * total[0] / total[1]

    @pl.loop(1, places)
    def _(k):
        send(out_ref.at[own], out_ref.at[own], out_send, out_recv, (peer(k) * 2 + core, r)).start()

    others = out_ref.at[pl.ds(0, (places - 1) * count)]
    gathered = send(others, others, out_send, out_recv, partner)
    gathered.wait_recv()
    last = send(out_ref.at[mine], out_ref.at[mine], last_send, last_recv, partner)
    last.start()
    last.wait_recv()
    for copy in (*copies, arrivals, gathered, last):
        copy.wait_send()


def template_call(mesh, cross, denominator, templates):
    ntm = mesh.shape["tm"]
    bins, k = templates.shape
    places = ntm // 2
    half = bins // 2
    whole = pl.BlockSpec(memory_space=VMEM)
    return pl.pallas_call(
        functools.partial(template_kernel, ntm),
        out_shape=jax.ShapeDtypeStruct((bins, k), F32),
        in_specs=[whole] * 3,
        out_specs=whole,
        scratch_shapes=[
            VMEM((2, half, k), F32),
            VMEM((2, half, k), F32),
            VMEM((places - 1, 2, half // places, k), F32),
            pltpu.SemaphoreType.DMA((2,)),
            pltpu.SemaphoreType.DMA((2,)),
            pltpu.SemaphoreType.DMA,
            pltpu.SemaphoreType.DMA,
            pltpu.SemaphoreType.DMA,
            pltpu.SemaphoreType.DMA,
            pltpu.SemaphoreType.DMA,
            pltpu.SemaphoreType.DMA,
        ],
        compiler_params=pltpu.CompilerParams(collective_id=1, has_side_effects=True),
        name="templates",
    )(cross, denominator, templates)


def body(mesh, spectrum, templates, activations, lengths):
    frames = spectrum.shape[1]
    tiles = (lengths + 7) // 8
    ends = jnp.cumsum(tiles)
    starts = ends - tiles
    index = jnp.arange(frames // 8, dtype=jnp.int32)
    gaps = TRACK_LEN // 8 - tiles
    src = index + jnp.sum(jnp.where(index[:, None] >= ends[None, :], gaps[None, :], 0), axis=1)
    src = jnp.minimum(src, frames // 8 - 1).astype(jnp.int32)
    count = jnp.broadcast_to(ends[-1].astype(F32), (8, 128))
    num, act, operand, most = numerator_call(mesh, spectrum, templates, activations, count)
    needed = most[0, 0] * 8.0
    branch = jnp.sum(needed > jnp.array(SIZES[:-1], F32)).astype(jnp.int32)
    branches = [functools.partial(refine_call, size, i) for i, size in enumerate(SIZES)]
    current = lax.switch(branch, branches, src, num, act, operand)
    new_activations, cross, denominator = cross_call(starts * 8, lengths, current, spectrum, templates)
    return new_activations, template_call(mesh, cross, denominator, templates)


def solution(mesh):
    return jax.shard_map(
        functools.partial(body, mesh),
        mesh=mesh,
        in_specs=(P("freq", "tm"), P("freq", None), P(None, "tm"), P("tm")),
        out_specs=(P(None, "tm"), P("freq", None)),
        check_vma=False,
    )
```

```python
import functools

import jax
import jax.numpy as jnp
from jax import lax
from jax.experimental import pallas as pl
from jax.experimental.pallas import tpu as pltpu
from jax.sharding import PartitionSpec as P

MESH = pl.DeviceIdType.MESH
TRACK_LEN = 512
UPDATES = 2
CHUNKS = 8
SIZES = (2048, 4096, 4608, 5120, 5632, 6144, 7168, 8192)
MIB = 1024 * 1024

F32 = jnp.float32
BF16 = jnp.bfloat16
VMEM = pltpu.VMEM


def split(x):
    high = x.astype(BF16)
    low = (x - high.astype(F32)).astype(BF16)
    return high, low


def right_operand(m):
    high, low = split(m)
    top = jnp.concatenate([high, low], axis=1)
    bottom = jnp.concatenate([high, jnp.zeros_like(low)], axis=1)
    return jnp.concatenate([top, bottom], axis=0)


def fine_dot(x, operand):
    high, low = split(x)
    both = jnp.dot(jnp.concatenate([high, low], axis=1), operand, preferred_element_type=F32)
    k = both.shape[1] // 2
    return both[:, :k] + both[:, k:]


def fold_quadrants(m):
    k = m.shape[0] // 2
    return (m[:k, :k] + m[k:, k:]) + (m[:k, k:] + m[k:, :k])


def on_hbm(x):
    return pltpu.with_memory_space_constraint(x, pltpu.HBM)


def send(src, dst, send_sem, recv_sem, device):
    return pltpu.make_async_remote_copy(
        src_ref=src, dst_ref=dst, send_sem=send_sem, recv_sem=recv_sem,
        device_id=device, device_id_type=MESH,
    )


def numerator_kernel(
    ntm, nfreq, steps, spec_hbm, templates_ref, act_hbm, lengths_ref,
    num_ref, act_out_ref, operand_ref, src_ref, branch_ref, spec,
    act, low_ref, gram_ref, grams_ref, count_ref, counts_ref,
    spec_sem, act_sem, gram_send, gram_recv, count_send, count_recv,
):
    t = lax.axis_index("tm")
    r = lax.axis_index("freq")

    barrier = pltpu.get_barrier_semaphore()

    @pl.loop(1, ntm)
    def _(k):
        pl.semaphore_signal(barrier, inc=1, device_id=(lax.rem(t + k, ntm), r), device_id_type=MESH)

    @pl.loop(1, nfreq)
    def _(k):
        pl.semaphore_signal(barrier, inc=1, device_id=(t, lax.rem(r + k, nfreq)), device_id_type=MESH)

    def columns(i):
        return pl.ds(pl.multiple_of(i * TRACK_LEN, TRACK_LEN), TRACK_LEN)

    def act_copy(i):
        return pltpu.make_async_copy(act_hbm.at[:, columns(i)], act.at[i], act_sem.at[i])

    def spec_copy(i):
        return pltpu.make_async_copy(spec_hbm.at[:, columns(i)], spec.at[i], spec_sem.at[i])

    @pl.loop(0, steps)
    def _(i):
        act_copy(i).start()

    @pl.loop(0, steps)
    def _(i):
        spec_copy(i).start()

    index = lax.broadcasted_iota(jnp.int32, (8, 128), 0) * 128 + lax.broadcasted_iota(jnp.int32, (8, 128), 1)
    table = index
    total = jnp.int32(0)
    per_track = TRACK_LEN // 8
    for j in range(steps):
        tiles = (lengths_ref[j] + 7) // 8
        total = total + tiles
        table = table + jnp.where(index >= total, per_track - tiles, 0)
    src_ref[...] = jnp.minimum(table, steps * per_track - 1)
    count_ref[...] = jnp.full((8, 128), total.astype(F32))

    turned = templates_ref[...].T
    high_t, low_t = split(turned)
    low_ref[...] = high_t
    high, low = split(templates_ref[...])
    products = jnp.dot(
        jnp.concatenate([high_t, low_t], axis=0),
        jnp.concatenate([high, low], axis=1),
        preferred_element_type=F32,
    )
    gram_ref[...] = fold_quadrants(products)

    @pl.loop(0, steps)
    def _(i):
        act_copy(i).wait()
        at = pl.ds(pl.multiple_of(i * per_track, per_track), per_track)
        act_out_ref[at] = act[i].T.reshape(per_track, 8, -1)

    pl.semaphore_wait(barrier, ntm + nfreq - 2)

    @pl.loop(1, ntm)
    def _(k):
        send(count_ref, counts_ref.at[k - 1], count_send, count_recv, (lax.rem(t + k, ntm), r)).start()

    def gram_copy(k):
        return send(gram_ref, grams_ref.at[k - 1], gram_send.at[k - 1], gram_recv.at[k - 1], (t, lax.rem(r + k, nfreq)))

    for k in range(1, nfreq):
        gram_copy(k).start()

    @pl.loop(0, steps)
    def _(i):
        spec_copy(i).wait()
        num = jnp.dot(low_ref[...], spec[i], preferred_element_type=F32)
        at = pl.ds(pl.multiple_of(i * per_track, per_track), per_track)
        num_ref[at] = num.T.reshape(per_track, 8, -1)

    everyone = send(counts_ref, counts_ref, count_send, count_recv, (lax.rem(t + 1, ntm), r))
    everyone.wait_send()
    everyone.wait_recv()
    most = count_ref[...]
    for k in range(ntm - 1):
        most = jnp.maximum(most, counts_ref[k])
    needed = jnp.max(most) * 8.0
    branch = jnp.int32(0)
    for size in SIZES[:-1]:
        branch = branch + (needed > size).astype(jnp.int32)
    branch_ref[0] = branch
    gram = gram_ref[...]
    for k in range(1, nfreq):
        gram_copy(k).wait_send()
        gram_copy(k).wait_recv()
        gram = gram + grams_ref[k - 1]
    operand_ref[...] = right_operand(gram)


def numerator_call(mesh, spectrum, templates, activations, lengths):
    ntm, nfreq = mesh.shape["tm"], mesh.shape["freq"]
    bins, frames = spectrum.shape
    k = templates.shape[1]
    steps = frames // TRACK_LEN
    whole = pl.BlockSpec(memory_space=VMEM)
    scalars = pl.BlockSpec(memory_space=pltpu.SMEM)
    far = pl.BlockSpec(memory_space=pltpu.HBM)
    return pl.pallas_call(
        functools.partial(numerator_kernel, ntm, nfreq, steps),
        out_shape=(
            VMEM((frames // 8, 8, k), F32),
            VMEM((frames // 8, 8, k), F32),
            jax.ShapeDtypeStruct((2 * k, 2 * k), BF16),
            jax.ShapeDtypeStruct((8, 128), jnp.int32),
            jax.ShapeDtypeStruct((1,), jnp.int32),
            VMEM((steps, bins, TRACK_LEN), BF16),
        ),
        in_specs=[far, whole, far, scalars],
        out_specs=(whole, whole, whole, whole, scalars, whole),
        scratch_shapes=[
            VMEM((steps, k, TRACK_LEN), F32),
            VMEM((k, bins), BF16),
            VMEM((k, k), F32),
            VMEM((nfreq - 1, k, k), F32),
            VMEM((8, 128), F32),
            VMEM((ntm - 1, 8, 128), F32),
            pltpu.SemaphoreType.DMA((steps,)),
            pltpu.SemaphoreType.DMA((steps,)),
            pltpu.SemaphoreType.DMA((nfreq - 1,)),
            pltpu.SemaphoreType.DMA((nfreq - 1,)),
            pltpu.SemaphoreType.DMA,
            pltpu.SemaphoreType.DMA,
        ],
        compiler_params=pltpu.CompilerParams(
            collective_id=0, has_side_effects=True, vmem_limit_bytes=8 * MIB,
        ),
        name="numerator",
    )(on_hbm(spectrum), templates, on_hbm(activations), lengths)


def refine_kernel(
    size, src_ref, num_ref, act_ref, operand_ref, out_ref,
    comp, own, first, direct, second, send_sem, first_sem, direct_sem, second_sem, near_sem, far_sem,
):
    t = lax.axis_index("tm")
    r = lax.axis_index("freq")
    shard, half = size // 4, size // 8
    cw = half // CHUNKS
    right, left, opposite = lax.rem(r + 1, 4), lax.rem(r + 3, 4), lax.rem(r + 2, 4)
    near = ((t, right), (t, left))

    barrier = pltpu.get_barrier_semaphore()
    for device in near:
        pl.semaphore_signal(barrier, inc=1, device_id=device, device_id_type=MESH)

    def rows(base, h, c):
        return pl.ds(pl.multiple_of(base * shard + h * half + c * cw, 8), cw)

    def part(c):
        return pl.ds(pl.multiple_of(c * cw, 8), cw)

    def gather(base, h, c, table, into, offset):
        start = base * shard + h * half + c * cw
        for i in range(cw // 8):
            tile = start // 8 + i
            source = src_ref[tile // 128, tile % 128]
            into[pl.ds(pl.multiple_of(start - offset + 8 * i, 8), 8), :] = table[source]

    def first_copy(way, c):
        return send(comp.at[rows(opposite, way, c)], first.at[way, part(c)], send_sem.at[way], first_sem.at[way, c], near[way])

    def direct_copy(way, c):
        return send(comp.at[rows((right, left)[way], 1 - way, c)], direct.at[way, part(c)], send_sem.at[2 + way], direct_sem.at[way, c], near[way])

    def second_copy(way, c):
        return send(first.at[way, part(c)], second.at[way, part(c)], send_sem.at[4 + way], second_sem.at[way, c], near[way])

    def near_copy(way, h, c):
        return send(out_ref.at[rows(r, h, c)], out_ref.at[rows(r, h, c)], send_sem.at[6 + 2 * way + h], near_sem.at[way, h, c], near[way])

    def near_arrival(way, h, c):
        owner = (left, right)[way]
        return send(out_ref.at[rows(owner, h, c)], out_ref.at[rows(owner, h, c)], send_sem.at[6 + 2 * way + h], near_sem.at[way, h, c], near[way])

    def far_copy(way, c):
        owner = (left, right)[way]
        return send(out_ref.at[rows(owner, way, c)], out_ref.at[rows(owner, way, c)], send_sem.at[10 + way], far_sem.at[way, c], near[way])

    def far_arrival(way, c):
        return send(out_ref.at[rows(opposite, way, c)], out_ref.at[rows(opposite, way, c)], send_sem.at[10 + way], far_sem.at[way, c], near[way])

    for way in range(2):
        gather(opposite, way, 0, num_ref, comp, 0)
    pl.semaphore_wait(barrier, 2)
    for way in range(2):
        first_copy(way, 0).start()

    @pl.loop(1, CHUNKS)
    def _(c):
        for way in range(2):
            gather(opposite, way, c, num_ref, comp, 0)
            first_copy(way, c).start()

    @pl.loop(0, CHUNKS)
    def _(c):
        for way in range(2):
            gather((right, left)[way], 1 - way, c, num_ref, comp, 0)
            direct_copy(way, c).start()

    @pl.loop(0, CHUNKS)
    def _(c):
        for way in range(2):
            gather((right, left)[way], way, c, num_ref, comp, 0)
            gather(r, way, c, num_ref, comp, 0)
            gather(r, way, c, act_ref, own, r * shard)

    @pl.loop(0, CHUNKS)
    def _(c):
        for way in range(2):
            first_copy(way, c).wait_recv()
            first[way, part(c), :] = first[way, part(c), :] + comp[rows((right, left)[way], way, c), :]
            second_copy(way, c).start()

    @pl.loop(0, CHUNKS)
    def _(c):
        for h in range(2):
            second_copy(h, c).wait_recv()
            direct_copy(1 - h, c).wait_recv()
            numerator = comp[rows(r, h, c), :] + second[h, part(c), :] + direct[1 - h, part(c), :]
            current = own[pl.ds(pl.multiple_of(h * half + c * cw, 8), cw), :]
            for _ in range(UPDATES):
                current = current * numerator / fine_dot(current, operand_ref[...])
            out_ref[rows(r, h, c), :] = current
            for way in range(2):
                near_copy(way, h, c).start()

    @pl.loop(0, CHUNKS)
    def _(c):
        for way in range(2):
            near_arrival(way, way, c).wait_recv()
            far_copy(way, c).start()

    @pl.loop(0, CHUNKS)
    def _(c):
        for way in range(2):
            near_arrival(way, 1 - way, c).wait_recv()
            far_arrival(way, c).wait_recv()

    for i in range(12):
        whole = first.at[0]
        send(whole, whole, send_sem.at[i], first_sem.at[0, 0], near[0]).wait_send()


def refine_call(size, index, src, num, act, operand):
    frames, k = num.shape[0] * 8, num.shape[2]
    shard, half = size // 4, size // 8
    whole = pl.BlockSpec(memory_space=VMEM)
    return pl.pallas_call(
        functools.partial(refine_kernel, size),
        out_shape=VMEM((frames, k), F32),
        in_specs=[pl.BlockSpec(memory_space=pltpu.SMEM), whole, whole, whole],
        out_specs=whole,
        scratch_shapes=[
            VMEM((size, k), F32),
            VMEM((shard, k), F32),
            VMEM((2, half, k), F32),
            VMEM((2, half, k), F32),
            VMEM((2, half, k), F32),
            pltpu.SemaphoreType.DMA((12,)),
            pltpu.SemaphoreType.DMA((2, CHUNKS)),
            pltpu.SemaphoreType.DMA((2, CHUNKS)),
            pltpu.SemaphoreType.DMA((2, CHUNKS)),
            pltpu.SemaphoreType.DMA((2, 2, CHUNKS)),
            pltpu.SemaphoreType.DMA((2, CHUNKS)),
        ],
        compiler_params=pltpu.CompilerParams(
            collective_id=2 + index, has_side_effects=True, vmem_limit_bytes=12 * MIB,
        ),
        name=f"refine_{size}",
    )(src, num, act, operand)


def cross_kernel(
    steps, lengths_ref, act_ref, spec, templates_ref, out_hbm, cross_ref, denominator_ref,
    turned_ref, gram_ref, out_sem,
):
    def columns(i):
        return pl.ds(pl.multiple_of(i * TRACK_LEN, TRACK_LEN), TRACK_LEN)

    def out_copy(i):
        return pltpu.make_async_copy(turned_ref.at[i], out_hbm.at[:, columns(i)], out_sem.at[i])

    gram_ref[...] = jnp.zeros_like(gram_ref)
    cross_ref[...] = jnp.zeros_like(cross_ref)

    def step(i, start):
        length = lengths_ref[i]
        x = act_ref[pl.ds(pl.multiple_of(start, 8), TRACK_LEN), :]
        position = lax.broadcasted_iota(jnp.int32, x.shape, 0)
        x = jnp.where(position < length, x, 0.0)
        turned = x.T
        turned_ref[i] = turned
        out_copy(i).start()
        high, low = split(x)
        high_t, low_t = split(turned)
        gram_ref[...] += jnp.dot(
            jnp.concatenate([high_t, low_t], axis=0),
            jnp.concatenate([high, low], axis=1),
            preferred_element_type=F32,
        )
        cross_ref[...] += jnp.dot(spec[i], high, preferred_element_type=F32)
        return start + (length + 7) // 8 * 8

    lax.fori_loop(0, steps, step, jnp.int32(0))
    denominator_ref[...] = fine_dot(templates_ref[...], right_operand(fold_quadrants(gram_ref[...])))

    @pl.loop(0, steps)
    def _(i):
        out_copy(i).wait()


def cross_call(lengths, act, spectrum, templates):
    steps, bins = spectrum.shape[:2]
    frames, k = act.shape
    whole = pl.BlockSpec(memory_space=VMEM)
    far = pl.BlockSpec(memory_space=pltpu.HBM)
    return pl.pallas_call(
        functools.partial(cross_kernel, steps),
        in_specs=[pl.BlockSpec(memory_space=pltpu.SMEM), whole, whole, whole],
        out_specs=(far, whole, whole),
        out_shape=(
            jax.ShapeDtypeStruct((k, frames), F32),
            jax.ShapeDtypeStruct((bins, k), F32),
            jax.ShapeDtypeStruct((bins, k), F32),
        ),
        scratch_shapes=[
            VMEM((steps, k, TRACK_LEN), F32),
            VMEM((2 * k, 2 * k), F32),
            pltpu.SemaphoreType.DMA((steps,)),
        ],
        compiler_params=pltpu.CompilerParams(vmem_limit_bytes=13 * MIB),
        name="cross",
    )(lengths, act, spectrum, templates)


def template_kernel(
    ntm, cross_ref, denominator_ref, templates_ref, out_ref,
    pair, acc, land, pair_send, pair_recv, land_send, land_recv, out_send, out_recv, last_send, last_recv,
):
    t = lax.axis_index("tm")
    r = lax.axis_index("freq")
    places = ntm // 2
    core = lax.rem(t, 2)
    place = t // 2
    partner = (place * 2 + 1 - core, r)
    half = cross_ref.shape[0] // 2
    count = half // places

    def peer(k):
        return lax.rem(place + k, places)

    barrier = pltpu.get_barrier_semaphore()
    pl.semaphore_signal(barrier, inc=1, device_id=partner, device_id_type=MESH)

    @pl.loop(1, places)
    def _(k):
        pl.semaphore_signal(barrier, inc=1, device_id=(peer(k) * 2 + core, r), device_id_type=MESH)

    pl.semaphore_wait(barrier, places)

    mine = pl.ds(pl.multiple_of(core * half, 8), half)
    theirs = pl.ds(pl.multiple_of((1 - core) * half, 8), half)
    copies = [
        send(ref.at[theirs], pair.at[i], pair_send.at[i], pair_recv.at[i], partner)
        for i, ref in enumerate((cross_ref, denominator_ref))
    ]
    for copy in copies:
        copy.start()
    for i, (copy, ref) in enumerate(zip(copies, (cross_ref, denominator_ref))):
        copy.wait_recv()
        acc[i] = ref[mine, :] + pair[i]

    def piece(k):
        rows = pl.ds(pl.multiple_of(peer(k) * count, 8), count)
        return send(acc.at[:, rows], land.at[k - 1], land_send, land_recv, (peer(k) * 2 + core, r))

    @pl.loop(1, places)
    def _(k):
        piece(k).start()

    arrivals = send(land, land, land_send, land_recv, partner)
    arrivals.wait_recv()
    rows = pl.ds(pl.multiple_of(place * count, 8), count)
    total = acc[:, rows, :]
    for k in range(1, places):
        total = total + land[k - 1]
    own = pl.ds(pl.multiple_of(core * half + place * count, 8), count)
    out_ref[own, :] = templates_ref[own, :] * total[0] / total[1]

    @pl.loop(1, places)
    def _(k):
        send(out_ref.at[own], out_ref.at[own], out_send, out_recv, (peer(k) * 2 + core, r)).start()

    others = out_ref.at[pl.ds(0, (places - 1) * count)]
    gathered = send(others, others, out_send, out_recv, partner)
    gathered.wait_recv()
    last = send(out_ref.at[mine], out_ref.at[mine], last_send, last_recv, partner)
    last.start()
    last.wait_recv()
    for copy in (*copies, arrivals, gathered, last):
        copy.wait_send()


def template_call(mesh, cross, denominator, templates):
    ntm = mesh.shape["tm"]
    bins, k = templates.shape
    places = ntm // 2
    half = bins // 2
    whole = pl.BlockSpec(memory_space=VMEM)
    return pl.pallas_call(
        functools.partial(template_kernel, ntm),
        out_shape=jax.ShapeDtypeStruct((bins, k), F32),
        in_specs=[whole] * 3,
        out_specs=whole,
        scratch_shapes=[
            VMEM((2, half, k), F32),
            VMEM((2, half, k), F32),
            VMEM((places - 1, 2, half // places, k), F32),
            pltpu.SemaphoreType.DMA((2,)),
            pltpu.SemaphoreType.DMA((2,)),
            pltpu.SemaphoreType.DMA,
            pltpu.SemaphoreType.DMA,
            pltpu.SemaphoreType.DMA,
            pltpu.SemaphoreType.DMA,
            pltpu.SemaphoreType.DMA,
            pltpu.SemaphoreType.DMA,
        ],
        compiler_params=pltpu.CompilerParams(collective_id=1, has_side_effects=True, vmem_limit_bytes=10 * MIB),
        name="templates",
    )(cross, denominator, templates)


def refine_and_cross(size, index, src, num, act, operand, lengths, spectrum, templates):
    current = refine_call(size, index, src, num, act, operand)
    return cross_call(lengths, current, spectrum, templates)


def body(mesh, spectrum, templates, activations, lengths):
    num, act, operand, src, branch, near_spectrum = numerator_call(mesh, spectrum, templates, activations, lengths)
    branches = [functools.partial(refine_and_cross, size, i) for i, size in enumerate(SIZES)]
    new_activations, cross, denominator = lax.switch(
        branch[0], branches, src, num, act, operand, lengths, near_spectrum, templates
    )
    return new_activations, template_call(mesh, cross, denominator, templates)


def solution(mesh):
    return jax.shard_map(
        functools.partial(body, mesh),
        mesh=mesh,
        in_specs=(P("freq", "tm"), P("freq", None), P(None, "tm"), P("tm")),
        out_specs=(P(None, "tm"), P("freq", None)),
        check_vma=False,
    )
```

```python
import functools

import jax
import jax.numpy as jnp
from jax import lax
from jax.experimental import pallas as pl
from jax.experimental.pallas import tpu as pltpu
from jax.sharding import PartitionSpec as P

MESH = pl.DeviceIdType.MESH
TRACK_LEN = 512
UPDATES = 2
AHEAD = 6
SIZES = (4096, 4928, 5184, 5376, 5632, 5824, 6272, 8192)
CHUNKS = (8, 7, 9, 7, 8, 7, 7, 8)
MIB = 1024 * 1024

F32 = jnp.float32
BF16 = jnp.bfloat16
VMEM = pltpu.VMEM


def split(x):
    high = x.astype(BF16)
    low = (x - high.astype(F32)).astype(BF16)
    return high, low


def right_operand(m):
    high, low = split(m)
    top = jnp.concatenate([high, low], axis=1)
    bottom = jnp.concatenate([high, jnp.zeros_like(low)], axis=1)
    return jnp.concatenate([top, bottom], axis=0)


def fine_dot(x, operand):
    high, low = split(x)
    both = jnp.dot(jnp.concatenate([high, low], axis=1), operand, preferred_element_type=F32)
    k = both.shape[1] // 2
    return both[:, :k] + both[:, k:]


def fold_quadrants(m):
    k = m.shape[0] // 2
    return (m[:k, :k] + m[k:, k:]) + (m[:k, k:] + m[k:, :k])


def on_hbm(x):
    return pltpu.with_memory_space_constraint(x, pltpu.HBM)


def send(src, dst, send_sem, recv_sem, device):
    return pltpu.make_async_remote_copy(
        src_ref=src, dst_ref=dst, send_sem=send_sem, recv_sem=recv_sem,
        device_id=device, device_id_type=MESH,
    )


def numerator_kernel(
    ntm, nfreq, steps, spec_hbm, templates_ref, act_hbm, lengths_ref,
    num_ref, act_out_ref, operand_ref, src_ref, branch_ref, spec,
    act, low_ref, gram_ref, grams_ref, count_ref, counts_ref,
    spec_sem, act_sem, gram_send, gram_recv, count_send, count_recv,
):
    t = lax.axis_index("tm")
    r = lax.axis_index("freq")

    barrier = pltpu.get_barrier_semaphore()

    @pl.loop(1, ntm)
    def _(k):
        pl.semaphore_signal(barrier, inc=1, device_id=(lax.rem(t + k, ntm), r), device_id_type=MESH)

    @pl.loop(1, nfreq)
    def _(k):
        pl.semaphore_signal(barrier, inc=1, device_id=(t, lax.rem(r + k, nfreq)), device_id_type=MESH)

    def columns(i):
        return pl.ds(pl.multiple_of(i * TRACK_LEN, TRACK_LEN), TRACK_LEN)

    def act_copy(i):
        return pltpu.make_async_copy(act_hbm.at[:, columns(i)], act.at[i], act_sem.at[i])

    def spec_copy(i):
        return pltpu.make_async_copy(spec_hbm.at[:, columns(i)], spec.at[i], spec_sem.at[i])

    @pl.loop(0, steps)
    def _(i):
        act_copy(i).start()

    @pl.loop(0, AHEAD)
    def _(i):
        spec_copy(i).start()

    index = lax.broadcasted_iota(jnp.int32, (8, 128), 0) * 128 + lax.broadcasted_iota(jnp.int32, (8, 128), 1)
    table = index
    total = jnp.int32(0)
    per_track = TRACK_LEN // 8
    for j in range(steps):
        tiles = (lengths_ref[j] + 7) // 8
        total = total + tiles
        table = table + jnp.where(index >= total, per_track - tiles, 0)
    src_ref[...] = jnp.minimum(table, steps * per_track - 1)
    count_ref[...] = jnp.full((8, 128), total.astype(F32))

    turned = templates_ref[...].T
    high_t, low_t = split(turned)
    low_ref[...] = high_t
    high, low = split(templates_ref[...])
    products = jnp.dot(
        jnp.concatenate([high_t, low_t], axis=0),
        jnp.concatenate([high, low], axis=1),
        preferred_element_type=F32,
    )
    gram_ref[...] = fold_quadrants(products)

    @pl.loop(0, steps)
    def _(i):
        act_copy(i).wait()
        at = pl.ds(pl.multiple_of(i * per_track, per_track), per_track)
        act_out_ref[at] = act[i].T.reshape(per_track, 8, -1)

    pl.semaphore_wait(barrier, ntm + nfreq - 2)

    def gram_copy(k):
        return send(gram_ref, grams_ref.at[k - 1], gram_send.at[k - 1], gram_recv.at[k - 1], (t, lax.rem(r + k, nfreq)))

    for k in range(1, nfreq):
        gram_copy(k).start()
    for k in range(1, ntm):
        send(count_ref, counts_ref.at[k - 1], count_send, count_recv, (lax.rem(t + k, ntm), r)).start()

    @pl.loop(0, steps)
    def _(i):
        spec_copy(i).wait()

        @pl.when(i + AHEAD < steps)
        def _():
            spec_copy(i + AHEAD).start()

        num = jnp.dot(low_ref[...], spec[i], preferred_element_type=F32)
        at = pl.ds(pl.multiple_of(i * per_track, per_track), per_track)
        num_ref[at] = num.T.reshape(per_track, 8, -1)

    everyone = send(counts_ref, counts_ref, count_send, count_recv, (lax.rem(t + 1, ntm), r))
    everyone.wait_send()
    everyone.wait_recv()
    most = count_ref[...]
    for k in range(ntm - 1):
        most = jnp.maximum(most, counts_ref[k])
    needed = jnp.max(most) * 8.0
    branch = jnp.int32(0)
    for size in SIZES[:-1]:
        branch = branch + (needed > size).astype(jnp.int32)
    branch_ref[0] = branch
    gram = gram_ref[...]
    for k in range(1, nfreq):
        gram_copy(k).wait_send()
        gram_copy(k).wait_recv()
        gram = gram + grams_ref[k - 1]
    operand_ref[...] = right_operand(gram)


def numerator_call(mesh, spectrum, templates, activations, lengths):
    ntm, nfreq = mesh.shape["tm"], mesh.shape["freq"]
    bins, frames = spectrum.shape
    k = templates.shape[1]
    steps = frames // TRACK_LEN
    whole = pl.BlockSpec(memory_space=VMEM)
    scalars = pl.BlockSpec(memory_space=pltpu.SMEM)
    far = pl.BlockSpec(memory_space=pltpu.HBM)
    return pl.pallas_call(
        functools.partial(numerator_kernel, ntm, nfreq, steps),
        out_shape=(
            VMEM((frames // 8, 8, k), F32),
            VMEM((frames // 8, 8, k), F32),
            jax.ShapeDtypeStruct((2 * k, 2 * k), BF16),
            jax.ShapeDtypeStruct((8, 128), jnp.int32),
            jax.ShapeDtypeStruct((1,), jnp.int32),
            VMEM((steps, bins, TRACK_LEN), BF16),
        ),
        in_specs=[far, whole, far, scalars],
        out_specs=(whole, whole, whole, whole, scalars, whole),
        scratch_shapes=[
            VMEM((steps, k, TRACK_LEN), F32),
            VMEM((k, bins), BF16),
            VMEM((k, k), F32),
            VMEM((nfreq - 1, k, k), F32),
            VMEM((8, 128), F32),
            VMEM((ntm - 1, 8, 128), F32),
            pltpu.SemaphoreType.DMA((steps,)),
            pltpu.SemaphoreType.DMA((steps,)),
            pltpu.SemaphoreType.DMA((nfreq - 1,)),
            pltpu.SemaphoreType.DMA((nfreq - 1,)),
            pltpu.SemaphoreType.DMA,
            pltpu.SemaphoreType.DMA,
        ],
        compiler_params=pltpu.CompilerParams(
            collective_id=0, has_side_effects=True, vmem_limit_bytes=8 * MIB,
        ),
        name="numerator",
    )(on_hbm(spectrum), templates, on_hbm(activations), lengths)


def refine_kernel(
    size, chunks, src_ref, num_ref, act_ref, operand_ref, out_ref,
    comp, own, first, direct, second, send_sem, first_sem, direct_sem, second_sem, near_sem, far_sem,
):
    t = lax.axis_index("tm")
    r = lax.axis_index("freq")
    shard, half = size // 4, size // 8
    cw = half // chunks
    right, left, opposite = lax.rem(r + 1, 4), lax.rem(r + 3, 4), lax.rem(r + 2, 4)
    near = ((t, right), (t, left))

    barrier = pltpu.get_barrier_semaphore()
    for device in near:
        pl.semaphore_signal(barrier, inc=1, device_id=device, device_id_type=MESH)

    def rows(base, h, c):
        return pl.ds(pl.multiple_of(base * shard + h * half + c * cw, 8), cw)

    def part(c):
        return pl.ds(pl.multiple_of(c * cw, 8), cw)

    def gather(base, h, c, table, into, offset):
        start = base * shard + h * half + c * cw
        for i in range(cw // 8):
            tile = start // 8 + i
            source = src_ref[tile // 128, tile % 128]
            into[pl.ds(pl.multiple_of(start - offset + 8 * i, 8), 8), :] = table[source]

    def first_copy(way, c):
        return send(comp.at[rows(opposite, way, c)], first.at[way, part(c)], send_sem.at[way], first_sem.at[way, c], near[way])

    def direct_copy(way, c):
        return send(comp.at[rows((right, left)[way], 1 - way, c)], direct.at[way, part(c)], send_sem.at[2 + way], direct_sem.at[way, c], near[way])

    def second_copy(way, c):
        return send(first.at[way, part(c)], second.at[way, part(c)], send_sem.at[4 + way], second_sem.at[way, c], near[way])

    def near_copy(way, h, c):
        return send(out_ref.at[rows(r, h, c)], out_ref.at[rows(r, h, c)], send_sem.at[6 + 2 * way + h], near_sem.at[way, h, c], near[way])

    def near_arrival(way, h, c):
        owner = (left, right)[way]
        return send(out_ref.at[rows(owner, h, c)], out_ref.at[rows(owner, h, c)], send_sem.at[6 + 2 * way + h], near_sem.at[way, h, c], near[way])

    def far_copy(way, c):
        owner = (left, right)[way]
        return send(out_ref.at[rows(owner, way, c)], out_ref.at[rows(owner, way, c)], send_sem.at[10 + way], far_sem.at[way, c], near[way])

    def far_arrival(way, c):
        return send(out_ref.at[rows(opposite, way, c)], out_ref.at[rows(opposite, way, c)], send_sem.at[10 + way], far_sem.at[way, c], near[way])

    for way in range(2):
        gather(opposite, way, 0, num_ref, comp, 0)
    pl.semaphore_wait(barrier, 2)
    for way in range(2):
        first_copy(way, 0).start()

    @pl.loop(1, chunks)
    def _(c):
        for way in range(2):
            gather(opposite, way, c, num_ref, comp, 0)
            first_copy(way, c).start()

    @pl.loop(0, chunks)
    def _(c):
        for way in range(2):
            gather((right, left)[way], 1 - way, c, num_ref, comp, 0)
            direct_copy(way, c).start()

    @pl.loop(0, chunks)
    def _(c):
        for way in range(2):
            gather((right, left)[way], way, c, num_ref, comp, 0)
            gather(r, way, c, num_ref, comp, 0)
            gather(r, way, c, act_ref, own, r * shard)

    @pl.loop(0, chunks)
    def _(c):
        for way in range(2):
            first_copy(way, c).wait_recv()
            first[way, part(c), :] = first[way, part(c), :] + comp[rows((right, left)[way], way, c), :]
            second_copy(way, c).start()

    @pl.loop(0, chunks)
    def _(c):
        for h in range(2):
            second_copy(h, c).wait_recv()
            direct_copy(1 - h, c).wait_recv()
            numerator = comp[rows(r, h, c), :] + second[h, part(c), :] + direct[1 - h, part(c), :]
            current = own[pl.ds(pl.multiple_of(h * half + c * cw, 8), cw), :]
            for _ in range(UPDATES):
                current = current * numerator / fine_dot(current, operand_ref[...])
            out_ref[rows(r, h, c), :] = current
            for way in range(2):
                near_copy(way, h, c).start()

    @pl.loop(0, chunks)
    def _(c):
        for way in range(2):
            near_arrival(way, way, c).wait_recv()
            far_copy(way, c).start()

    @pl.loop(0, chunks)
    def _(c):
        for way in range(2):
            near_arrival(way, 1 - way, c).wait_recv()
            far_arrival(way, c).wait_recv()

    for i in range(12):
        whole = first.at[0]
        send(whole, whole, send_sem.at[i], first_sem.at[0, 0], near[0]).wait_send()


def refine_call(size, index, src, num, act, operand):
    frames, k = num.shape[0] * 8, num.shape[2]
    shard, half = size // 4, size // 8
    chunks = CHUNKS[index]
    whole = pl.BlockSpec(memory_space=VMEM)
    return pl.pallas_call(
        functools.partial(refine_kernel, size, chunks),
        out_shape=VMEM((frames, k), F32),
        in_specs=[pl.BlockSpec(memory_space=pltpu.SMEM), whole, whole, whole],
        out_specs=whole,
        scratch_shapes=[
            VMEM((size, k), F32),
            VMEM((shard, k), F32),
            VMEM((2, half, k), F32),
            VMEM((2, half, k), F32),
            VMEM((2, half, k), F32),
            pltpu.SemaphoreType.DMA((12,)),
            pltpu.SemaphoreType.DMA((2, chunks)),
            pltpu.SemaphoreType.DMA((2, chunks)),
            pltpu.SemaphoreType.DMA((2, chunks)),
            pltpu.SemaphoreType.DMA((2, 2, chunks)),
            pltpu.SemaphoreType.DMA((2, chunks)),
        ],
        compiler_params=pltpu.CompilerParams(
            collective_id=1 + index, has_side_effects=True, vmem_limit_bytes=12 * MIB,
        ),
        name=f"refine_{size}",
    )(src, num, act, operand)


def template_kernel(
    steps, lengths_ref, act_ref, spec, templates_ref, placed_ref, out_ref,
    high_ref, denominator_ref, expanded, gram_ref, stage, pair, den_pair, land, den_land,
    stage_send, pair_recv, den_pair_send, den_pair_recv, land_send, land_recv, den_send, den_recv,
    out_send, out_recv, last_send, last_recv,
):
    t = lax.axis_index("tm")
    r = lax.axis_index("freq")
    core = lax.rem(t, 2)
    y = lax.rem(t // 2, 4)
    z = t // 8
    bins = templates_ref.shape[0]
    half = bins // 2
    block = bins // 8
    count = block // 4
    partner = (t + 1 - 2 * core, r)
    def there(q):
        return lax.rem(z + q, 4)

    def device(q, s):
        return ((there(q) * 4 + lax.rem(y + s, 4)) * 2 + core, r)

    def each_peer(do):
        @pl.loop(1, 16)
        def _(k):
            do(k // 4, lax.rem(k, 4))

    barrier = pltpu.get_barrier_semaphore()
    pl.semaphore_signal(barrier, inc=1, device_id=partner, device_id_type=MESH)
    each_peer(lambda q, s: pl.semaphore_signal(barrier, inc=1, device_id=device(q, s), device_id_type=MESH))

    gram_ref[...] = jnp.zeros_like(gram_ref)
    position = lax.broadcasted_iota(jnp.int32, (8, templates_ref.shape[1]), 0)

    def place(i, start):
        length = lengths_ref[i]
        for j in range(TRACK_LEN // 8):
            expanded[8 * j : 8 * j + 8, :] = jnp.where(position + 8 * j < length, act_ref[start + j], 0.0)
        x = expanded[...]
        turned = x.T
        placed_ref[:, pl.ds(pl.multiple_of(i * TRACK_LEN, TRACK_LEN), TRACK_LEN)] = turned
        high, low = split(x)
        high_ref[i] = high
        high_t, low_t = split(turned)
        gram_ref[...] += jnp.dot(
            jnp.concatenate([high_t, low_t], axis=0),
            jnp.concatenate([high, low], axis=1),
            preferred_element_type=F32,
        )
        return start + (length + 7) // 8

    lax.fori_loop(0, steps, place, jnp.int32(0))
    denominator_ref[...] = fine_dot(templates_ref[...], right_operand(fold_quadrants(gram_ref[...])))
    pl.semaphore_wait(barrier, 16)

    theirs = pl.ds(pl.multiple_of((1 - core) * half, half), half)
    mine = pl.ds(pl.multiple_of(core * half, half), half)
    den_copy = send(denominator_ref.at[theirs], den_pair, den_pair_send, den_pair_recv, partner)
    den_copy.start()

    def pair_copy(q):
        return send(stage.at[0, q], pair.at[q], stage_send.at[q], pair_recv.at[q], partner)

    def piece(s):
        return pl.ds(pl.multiple_of(lax.rem(y + s, 4) * count, count), count)

    def den_piece(q, s):
        at = pl.ds(pl.multiple_of(there(q) * block + lax.rem(y + s, 4) * count, count), count)
        return send(den_pair.at[at], den_land.at[q * 4 + s - 1], den_send, den_recv, device(q, s))

    def cross_piece(q, s):
        return send(stage.at[1, q, piece(s)], land.at[q * 4 + s - 1], land_send, land_recv, device(q, s))

    @pl.loop(0, 8)
    def _(n):
        own_side = n // 4
        q = lax.rem(n + 1, 4)
        side = lax.rem(core + 1 + own_side, 2)
        rows = pl.ds(pl.multiple_of((side * 4 + there(q)) * block, block), block)
        total = jnp.dot(spec[0, rows, :], high_ref[0], preferred_element_type=F32)
        for i in range(1, steps):
            total = total + jnp.dot(spec[i, rows, :], high_ref[i], preferred_element_type=F32)
        stage[own_side, q] = total

        @pl.when(n < 4)
        def _():
            pair_copy(q).start()

        @pl.when(n == 1)
        def _():
            den_copy.wait()
            den_pair[...] = den_pair[...] + denominator_ref[mine, :]
            each_peer(lambda q, s: den_piece(q, s).start())

        @pl.when(n >= 4)
        def _():
            pair_copy(q).wait_recv()
            stage[1, q] = stage[1, q] + pair[q]
            for s in (1, 2, 3):
                cross_piece(q, s).start()

            @pl.when(q > 0)
            def _():
                cross_piece(q, 0).start()

    den_all = send(den_land, den_land, den_send, den_recv, partner)
    cross_all = send(land, land, land_send, land_recv, partner)
    den_all.wait_recv()
    offset = z * block + y * count
    denominator = den_pair[pl.ds(pl.multiple_of(offset, count), count), :]
    for k in range(15):
        denominator = denominator + den_land[k]
    cross_all.wait_recv()
    cross = stage[1, 0, piece(0), :]
    for k in range(15):
        cross = cross + land[k]
    own = pl.ds(pl.multiple_of(core * half + offset, count), count)
    out_ref[own, :] = templates_ref[own, :] * cross / denominator

    each_peer(lambda q, s: send(out_ref.at[own], out_ref.at[own], out_send, out_recv, device(q, s)).start())

    others = out_ref.at[pl.ds(0, 15 * count)]
    gathered = send(others, others, out_send, out_recv, partner)
    gathered.wait_recv()
    last = send(out_ref.at[mine], out_ref.at[mine], last_send, last_recv, partner)
    last.start()
    last.wait_recv()
    for q in range(4):
        pair_copy(q).wait_send()
    for copy in (den_all, cross_all, gathered, last):
        copy.wait_send()


def template_call(index, lengths, act, spectrum, templates):
    bins, k = templates.shape
    steps = spectrum.shape[0]
    half, block, count = bins // 2, bins // 8, bins // 32
    whole = pl.BlockSpec(memory_space=VMEM)
    one = pltpu.SemaphoreType.DMA
    return pl.pallas_call(
        functools.partial(template_kernel, steps),
        out_shape=(VMEM((k, steps * TRACK_LEN), F32), jax.ShapeDtypeStruct((bins, k), F32)),
        in_specs=[pl.BlockSpec(memory_space=pltpu.SMEM)] + [whole] * 3,
        out_specs=(whole, whole),
        scratch_shapes=[
            VMEM((steps, TRACK_LEN, k), BF16),
            VMEM((bins, k), F32),
            VMEM((TRACK_LEN, k), F32),
            VMEM((2 * k, 2 * k), F32),
            VMEM((2, 4, block, k), F32),
            VMEM((4, block, k), F32),
            VMEM((half, k), F32),
            VMEM((15, count, k), F32),
            VMEM((15, count, k), F32),
            one((4,)), one((4,)), one, one, one, one, one, one, one, one, one, one,
        ],
        compiler_params=pltpu.CompilerParams(
            collective_id=1 + len(SIZES) + index, has_side_effects=True, vmem_limit_bytes=8 * MIB
        ),
        name=f"templates_{index}",
    )(lengths, act, spectrum, templates)


def store_kernel(placed_ref, out_hbm, sem):
    k = placed_ref.shape[0]
    parts = 8
    copies = []
    for i in range(parts):
        rows = pl.ds(i * (k // parts), k // parts)
        copies.append(pltpu.make_async_copy(placed_ref.at[rows], out_hbm.at[rows], sem.at[i]))
    for copy in copies:
        copy.start()
    for copy in copies:
        copy.wait()


def store_call(placed):
    return pl.pallas_call(
        store_kernel,
        out_shape=jax.ShapeDtypeStruct(placed.shape, placed.dtype),
        in_specs=[pl.BlockSpec(memory_space=VMEM)],
        out_specs=pl.BlockSpec(memory_space=pltpu.HBM),
        scratch_shapes=[pltpu.SemaphoreType.DMA((8,))],
        compiler_params=pltpu.CompilerParams(vmem_limit_bytes=5 * MIB),
        name="store",
    )(placed)


def rest(size, index, src, num, act, operand, lengths, spectrum, templates):
    current = refine_call(size, index, src, num, act, operand)
    current = current.reshape(current.shape[0] // 8, 8, -1)
    placed, new_templates = template_call(index, lengths, current, spectrum, templates)
    return store_call(placed), new_templates


def body(mesh, spectrum, templates, activations, lengths):
    num, act, operand, src, branch, near_spectrum = numerator_call(mesh, spectrum, templates, activations, lengths)
    branches = [functools.partial(rest, size, i) for i, size in enumerate(SIZES)]
    return lax.switch(branch[0], branches, src, num, act, operand, lengths, near_spectrum, templates)


def solution(mesh):
    return jax.shard_map(
        functools.partial(body, mesh),
        mesh=mesh,
        in_specs=(P("freq", "tm"), P("freq", None), P(None, "tm"), P("tm")),
        out_specs=(P(None, "tm"), P("freq", None)),
        check_vma=False,
    )
```

```python
import functools

import jax
import jax.numpy as jnp
from jax import lax
from jax.experimental import pallas as pl
from jax.experimental.pallas import tpu as pltpu
from jax.sharding import PartitionSpec as P

MESH = pl.DeviceIdType.MESH
TRACK_LEN = 512
UPDATES = 2
AHEAD = 6
SIZES = (4096, 4928, 5184, 5376, 5632, 5824, 6272, 8192)
CHUNKS = (8, 7, 9, 7, 8, 7, 7, 8)
MIB = 1024 * 1024

F32 = jnp.float32
BF16 = jnp.bfloat16
VMEM = pltpu.VMEM


def split(x):
    high = x.astype(BF16)
    low = (x - high.astype(F32)).astype(BF16)
    return high, low


def right_operand(m):
    high, low = split(m)
    top = jnp.concatenate([high, low], axis=1)
    bottom = jnp.concatenate([high, jnp.zeros_like(low)], axis=1)
    return jnp.concatenate([top, bottom], axis=0)


def fine_dot(x, operand):
    high, low = split(x)
    both = jnp.dot(jnp.concatenate([high, low], axis=1), operand, preferred_element_type=F32)
    k = both.shape[1] // 2
    return both[:, :k] + both[:, k:]


def fold_quadrants(m):
    k = m.shape[0] // 2
    return (m[:k, :k] + m[k:, k:]) + (m[:k, k:] + m[k:, :k])


def on_hbm(x):
    return pltpu.with_memory_space_constraint(x, pltpu.HBM)


def send(src, dst, send_sem, recv_sem, device):
    return pltpu.make_async_remote_copy(
        src_ref=src, dst_ref=dst, send_sem=send_sem, recv_sem=recv_sem,
        device_id=device, device_id_type=MESH,
    )


def numerator_kernel(
    ntm, nfreq, steps, spec_hbm, templates_hbm, act_hbm, lengths_ref,
    num_ref, act_out_ref, operand_ref, src_ref, branch_ref, spec,
    act, templates_ref, low_ref, gram_ref, grams_ref, count_ref, counts_ref,
    templates_sem, spec_sem, act_sem, gram_send, gram_recv, count_send, count_recv,
):
    t = lax.axis_index("tm")
    r = lax.axis_index("freq")

    def columns(i):
        return pl.ds(pl.multiple_of(i * TRACK_LEN, TRACK_LEN), TRACK_LEN)

    def act_copy(i):
        return pltpu.make_async_copy(act_hbm.at[:, columns(i)], act.at[i], act_sem.at[i])

    def spec_copy(i):
        return pltpu.make_async_copy(spec_hbm.at[:, columns(i)], spec.at[i], spec_sem.at[i])

    templates_copy = pltpu.make_async_copy(templates_hbm, templates_ref, templates_sem)
    templates_copy.start()

    @pl.loop(0, AHEAD)
    def _(i):
        act_copy(i).start()
        spec_copy(i).start()

    @pl.loop(AHEAD, steps)
    def _(i):
        act_copy(i).start()

    barrier = pltpu.get_barrier_semaphore()

    @pl.loop(1, ntm)
    def _(k):
        pl.semaphore_signal(barrier, inc=1, device_id=(lax.rem(t + k, ntm), r), device_id_type=MESH)

    @pl.loop(1, nfreq)
    def _(k):
        pl.semaphore_signal(barrier, inc=1, device_id=(t, lax.rem(r + k, nfreq)), device_id_type=MESH)

    index = lax.broadcasted_iota(jnp.int32, (8, 128), 0) * 128 + lax.broadcasted_iota(jnp.int32, (8, 128), 1)
    table = index
    total = jnp.int32(0)
    per_track = TRACK_LEN // 8
    for j in range(steps):
        tiles = (lengths_ref[j] + 7) // 8
        total = total + tiles
        table = table + jnp.where(index >= total, per_track - tiles, 0)
    src_ref[...] = jnp.minimum(table, steps * per_track - 1)
    count_ref[...] = jnp.full((8, 128), total.astype(F32))

    templates_copy.wait()
    turned = templates_ref[...].T
    high_t, low_t = split(turned)
    low_ref[...] = high_t
    high, low = split(templates_ref[...])
    products = jnp.dot(
        jnp.concatenate([high_t, low_t], axis=0),
        jnp.concatenate([high, low], axis=1),
        preferred_element_type=F32,
    )
    gram_ref[...] = fold_quadrants(products)

    def gram_copy(k):
        return send(gram_ref, grams_ref.at[k - 1], gram_send.at[k - 1], gram_recv.at[k - 1], (t, lax.rem(r + k, nfreq)))

    @pl.loop(0, steps)
    def _(i):
        spec_copy(i).wait()

        @pl.when(i + AHEAD < steps)
        def _():
            spec_copy(i + AHEAD).start()

        act_copy(i).wait()
        num = jnp.dot(low_ref[...], spec[i], preferred_element_type=F32)
        at = pl.ds(pl.multiple_of(i * per_track, per_track), per_track)
        num_ref[at] = num.T.reshape(per_track, 8, -1)
        act_out_ref[at] = act[i].T.reshape(per_track, 8, -1)

        @pl.when(i == 3)
        def _():
            pl.semaphore_wait(barrier, ntm + nfreq - 2)
            for k in range(1, nfreq):
                gram_copy(k).start()

            @pl.loop(1, ntm)
            def _(k):
                send(count_ref, counts_ref.at[k - 1], count_send, count_recv, (lax.rem(t + k, ntm), r)).start()

    everyone = send(counts_ref, counts_ref, count_send, count_recv, (lax.rem(t + 1, ntm), r))
    everyone.wait_send()
    everyone.wait_recv()
    most = count_ref[...]
    for k in range(ntm - 1):
        most = jnp.maximum(most, counts_ref[k])
    needed = jnp.max(most) * 8.0
    branch = jnp.int32(0)
    for size in SIZES[:-1]:
        branch = branch + (needed > size).astype(jnp.int32)
    branch_ref[0] = branch
    gram = gram_ref[...]
    for k in range(1, nfreq):
        gram_copy(k).wait_send()
        gram_copy(k).wait_recv()
        gram = gram + grams_ref[k - 1]
    operand_ref[...] = right_operand(gram)


def numerator_call(mesh, spectrum, templates, activations, lengths):
    ntm, nfreq = mesh.shape["tm"], mesh.shape["freq"]
    bins, frames = spectrum.shape
    k = templates.shape[1]
    steps = frames // TRACK_LEN
    whole = pl.BlockSpec(memory_space=VMEM)
    scalars = pl.BlockSpec(memory_space=pltpu.SMEM)
    far = pl.BlockSpec(memory_space=pltpu.HBM)
    return pl.pallas_call(
        functools.partial(numerator_kernel, ntm, nfreq, steps),
        out_shape=(
            VMEM((frames // 8, 8, k), F32),
            VMEM((frames // 8, 8, k), F32),
            jax.ShapeDtypeStruct((2 * k, 2 * k), BF16),
            jax.ShapeDtypeStruct((8, 128), jnp.int32),
            jax.ShapeDtypeStruct((1,), jnp.int32),
            VMEM((steps, bins, TRACK_LEN), BF16),
        ),
        in_specs=[far, far, far, scalars],
        out_specs=(whole, whole, whole, whole, scalars, whole),
        scratch_shapes=[
            VMEM((steps, k, TRACK_LEN), F32),
            VMEM((bins, k), F32),
            VMEM((k, bins), BF16),
            VMEM((k, k), F32),
            VMEM((nfreq - 1, k, k), F32),
            VMEM((8, 128), F32),
            VMEM((ntm - 1, 8, 128), F32),
            pltpu.SemaphoreType.DMA,
            pltpu.SemaphoreType.DMA((steps,)),
            pltpu.SemaphoreType.DMA((steps,)),
            pltpu.SemaphoreType.DMA((nfreq - 1,)),
            pltpu.SemaphoreType.DMA((nfreq - 1,)),
            pltpu.SemaphoreType.DMA,
            pltpu.SemaphoreType.DMA,
        ],
        compiler_params=pltpu.CompilerParams(
            collective_id=0, has_side_effects=True, vmem_limit_bytes=8 * MIB,
        ),
        name="numerator",
    )(on_hbm(spectrum), on_hbm(templates), on_hbm(activations), lengths)


def refine_kernel(
    size, chunks, src_ref, num_ref, act_ref, operand_ref, out_ref,
    comp, own, first, direct, second, send_sem, first_sem, direct_sem, second_sem, near_sem, far_sem,
):
    t = lax.axis_index("tm")
    r = lax.axis_index("freq")
    shard, half = size // 4, size // 8
    cw = half // chunks
    right, left, opposite = lax.rem(r + 1, 4), lax.rem(r + 3, 4), lax.rem(r + 2, 4)
    near = ((t, right), (t, left))

    barrier = pltpu.get_barrier_semaphore()
    for device in near:
        pl.semaphore_signal(barrier, inc=1, device_id=device, device_id_type=MESH)

    def rows(base, h, c):
        return pl.ds(pl.multiple_of(base * shard + h * half + c * cw, 8), cw)

    def part(c):
        return pl.ds(pl.multiple_of(c * cw, 8), cw)

    def gather(base, h, c, table, into, offset):
        start = base * shard + h * half + c * cw
        for i in range(cw // 8):
            tile = start // 8 + i
            source = src_ref[tile // 128, tile % 128]
            into[pl.ds(pl.multiple_of(start - offset + 8 * i, 8), 8), :] = table[source]

    def first_copy(way, c):
        return send(comp.at[rows(opposite, way, c)], first.at[way, part(c)], send_sem.at[way], first_sem.at[way, c], near[way])

    def direct_copy(way, c):
        return send(comp.at[rows((right, left)[way], 1 - way, c)], direct.at[way, part(c)], send_sem.at[2 + way], direct_sem.at[way, c], near[way])

    def second_copy(way, c):
        return send(first.at[way, part(c)], second.at[way, part(c)], send_sem.at[4 + way], second_sem.at[way, c], near[way])

    def near_copy(way, h, c):
        return send(out_ref.at[rows(r, h, c)], out_ref.at[rows(r, h, c)], send_sem.at[6 + 2 * way + h], near_sem.at[way, h, c], near[way])

    def near_arrival(way, h, c):
        owner = (left, right)[way]
        return send(out_ref.at[rows(owner, h, c)], out_ref.at[rows(owner, h, c)], send_sem.at[6 + 2 * way + h], near_sem.at[way, h, c], near[way])

    def far_copy(way, c):
        owner = (left, right)[way]
        return send(out_ref.at[rows(owner, way, c)], out_ref.at[rows(owner, way, c)], send_sem.at[10 + way], far_sem.at[way, c], near[way])

    def far_arrival(way, c):
        return send(out_ref.at[rows(opposite, way, c)], out_ref.at[rows(opposite, way, c)], send_sem.at[10 + way], far_sem.at[way, c], near[way])

    for way in range(2):
        gather(opposite, way, 0, num_ref, comp, 0)
    pl.semaphore_wait(barrier, 2)
    for way in range(2):
        first_copy(way, 0).start()

    @pl.loop(1, chunks)
    def _(c):
        for way in range(2):
            gather(opposite, way, c, num_ref, comp, 0)
            first_copy(way, c).start()

    @pl.loop(0, chunks)
    def _(c):
        for way in range(2):
            gather((right, left)[way], 1 - way, c, num_ref, comp, 0)
            direct_copy(way, c).start()

    @pl.loop(0, chunks)
    def _(c):
        for way in range(2):
            gather((right, left)[way], way, c, num_ref, comp, 0)
            gather(r, way, c, num_ref, comp, 0)
            gather(r, way, c, act_ref, own, r * shard)

    @pl.loop(0, chunks)
    def _(c):
        for way in range(2):
            first_copy(way, c).wait_recv()
            first[way, part(c), :] = first[way, part(c), :] + comp[rows((right, left)[way], way, c), :]
            second_copy(way, c).start()

    @pl.loop(0, chunks)
    def _(c):
        for h in range(2):
            second_copy(h, c).wait_recv()
            direct_copy(1 - h, c).wait_recv()
            numerator = comp[rows(r, h, c), :] + second[h, part(c), :] + direct[1 - h, part(c), :]
            current = own[pl.ds(pl.multiple_of(h * half + c * cw, 8), cw), :]
            for _ in range(UPDATES):
                current = current * numerator / fine_dot(current, operand_ref[...])
            out_ref[rows(r, h, c), :] = current
            for way in range(2):
                near_copy(way, h, c).start()

    @pl.loop(0, chunks)
    def _(c):
        for way in range(2):
            near_arrival(way, way, c).wait_recv()
            far_copy(way, c).start()

    @pl.loop(0, chunks)
    def _(c):
        for way in range(2):
            near_arrival(way, 1 - way, c).wait_recv()
            far_arrival(way, c).wait_recv()

    for i in range(12):
        whole = first.at[0]
        send(whole, whole, send_sem.at[i], first_sem.at[0, 0], near[0]).wait_send()


def refine_call(size, index, src, num, act, operand):
    frames, k = num.shape[0] * 8, num.shape[2]
    shard, half = size // 4, size // 8
    chunks = CHUNKS[index]
    whole = pl.BlockSpec(memory_space=VMEM)
    return pl.pallas_call(
        functools.partial(refine_kernel, size, chunks),
        out_shape=VMEM((frames, k), F32),
        in_specs=[pl.BlockSpec(memory_space=pltpu.SMEM), whole, whole, whole],
        out_specs=whole,
        scratch_shapes=[
            VMEM((size, k), F32),
            VMEM((shard, k), F32),
            VMEM((2, half, k), F32),
            VMEM((2, half, k), F32),
            VMEM((2, half, k), F32),
            pltpu.SemaphoreType.DMA((12,)),
            pltpu.SemaphoreType.DMA((2, chunks)),
            pltpu.SemaphoreType.DMA((2, chunks)),
            pltpu.SemaphoreType.DMA((2, chunks)),
            pltpu.SemaphoreType.DMA((2, 2, chunks)),
            pltpu.SemaphoreType.DMA((2, chunks)),
        ],
        compiler_params=pltpu.CompilerParams(
            collective_id=1 + index, has_side_effects=True, vmem_limit_bytes=12 * MIB,
        ),
        name=f"refine_{size}",
    )(src, num, act, operand)


def template_kernel(
    steps, lengths_ref, act_ref, spec, templates_ref, placed_ref, out_ref,
    high_ref, denominator_ref, expanded, gram_ref, stage, pair, den_pair, land, den_land,
    stage_send, pair_recv, den_pair_send, den_pair_recv, land_send, land_recv, den_send, den_recv,
    out_send, out_recv, last_send, last_recv,
):
    t = lax.axis_index("tm")
    r = lax.axis_index("freq")
    core = lax.rem(t, 2)
    y = lax.rem(t // 2, 4)
    z = t // 8
    bins = templates_ref.shape[0]
    half = bins // 2
    block = bins // 8
    count = block // 4
    partner = (t + 1 - 2 * core, r)
    def there(q):
        return lax.rem(z + q, 4)

    def device(q, s):
        return ((there(q) * 4 + lax.rem(y + s, 4)) * 2 + core, r)

    def each_peer(do):
        @pl.loop(1, 16)
        def _(k):
            do(k // 4, lax.rem(k, 4))

    barrier = pltpu.get_barrier_semaphore()
    pl.semaphore_signal(barrier, inc=1, device_id=partner, device_id_type=MESH)
    each_peer(lambda q, s: pl.semaphore_signal(barrier, inc=1, device_id=device(q, s), device_id_type=MESH))

    gram_ref[...] = jnp.zeros_like(gram_ref)
    position = lax.broadcasted_iota(jnp.int32, (8, templates_ref.shape[1]), 0)

    def place(i, start):
        length = lengths_ref[i]
        for j in range(TRACK_LEN // 8):
            expanded[8 * j : 8 * j + 8, :] = jnp.where(position + 8 * j < length, act_ref[start + j], 0.0)
        x = expanded[...]
        turned = x.T
        placed_ref[:, pl.ds(pl.multiple_of(i * TRACK_LEN, TRACK_LEN), TRACK_LEN)] = turned
        high, low = split(x)
        high_ref[i] = high
        high_t, low_t = split(turned)
        gram_ref[...] += jnp.dot(
            jnp.concatenate([high_t, low_t], axis=0),
            jnp.concatenate([high, low], axis=1),
            preferred_element_type=F32,
        )
        return start + (length + 7) // 8

    lax.fori_loop(0, steps, place, jnp.int32(0))
    denominator_ref[...] = fine_dot(templates_ref[...], right_operand(fold_quadrants(gram_ref[...])))
    pl.semaphore_wait(barrier, 16)

    theirs = pl.ds(pl.multiple_of((1 - core) * half, half), half)
    mine = pl.ds(pl.multiple_of(core * half, half), half)
    den_copy = send(denominator_ref.at[theirs], den_pair, den_pair_send, den_pair_recv, partner)
    den_copy.start()

    def pair_copy(q):
        return send(stage.at[0, q], pair.at[q], stage_send.at[q], pair_recv.at[q], partner)

    def piece(s):
        return pl.ds(pl.multiple_of(lax.rem(y + s, 4) * count, count), count)

    def den_piece(q, s):
        at = pl.ds(pl.multiple_of(there(q) * block + lax.rem(y + s, 4) * count, count), count)
        return send(den_pair.at[at], den_land.at[q * 4 + s - 1], den_send, den_recv, device(q, s))

    def cross_piece(q, s):
        return send(stage.at[1, q, piece(s)], land.at[q * 4 + s - 1], land_send, land_recv, device(q, s))

    @pl.loop(0, 8)
    def _(n):
        own_side = n // 4
        q = lax.rem(n + 1, 4)
        side = lax.rem(core + 1 + own_side, 2)
        rows = pl.ds(pl.multiple_of((side * 4 + there(q)) * block, block), block)
        total = jnp.dot(spec[0, rows, :], high_ref[0], preferred_element_type=F32)
        for i in range(1, steps):
            total = total + jnp.dot(spec[i, rows, :], high_ref[i], preferred_element_type=F32)
        stage[own_side, q] = total

        @pl.when(n < 4)
        def _():
            pair_copy(q).start()

        @pl.when(n == 1)
        def _():
            den_copy.wait()
            den_pair[...] = den_pair[...] + denominator_ref[mine, :]
            each_peer(lambda q, s: den_piece(q, s).start())

        @pl.when(n >= 4)
        def _():
            pair_copy(q).wait_recv()
            stage[1, q] = stage[1, q] + pair[q]
            for s in (1, 2, 3):
                cross_piece(q, s).start()

            @pl.when(q > 0)
            def _():
                cross_piece(q, 0).start()

    den_all = send(den_land, den_land, den_send, den_recv, partner)
    cross_all = send(land, land, land_send, land_recv, partner)
    den_all.wait_recv()
    offset = z * block + y * count
    denominator = den_pair[pl.ds(pl.multiple_of(offset, count), count), :]
    for k in range(15):
        denominator = denominator + den_land[k]
    cross_all.wait_recv()
    cross = stage[1, 0, piece(0), :]
    for k in range(15):
        cross = cross + land[k]
    own = pl.ds(pl.multiple_of(core * half + offset, count), count)
    out_ref[own, :] = templates_ref[own, :] * cross / denominator

    each_peer(lambda q, s: send(out_ref.at[own], out_ref.at[own], out_send, out_recv, device(q, s)).start())

    others = out_ref.at[pl.ds(0, 15 * count)]
    gathered = send(others, others, out_send, out_recv, partner)
    gathered.wait_recv()
    last = send(out_ref.at[mine], out_ref.at[mine], last_send, last_recv, partner)
    last.start()
    last.wait_recv()
    for q in range(4):
        pair_copy(q).wait_send()
    for copy in (den_all, cross_all, gathered, last):
        copy.wait_send()


def template_call(index, lengths, act, spectrum, templates):
    bins, k = templates.shape
    steps = spectrum.shape[0]
    half, block, count = bins // 2, bins // 8, bins // 32
    whole = pl.BlockSpec(memory_space=VMEM)
    one = pltpu.SemaphoreType.DMA
    return pl.pallas_call(
        functools.partial(template_kernel, steps),
        out_shape=(VMEM((k, steps * TRACK_LEN), F32), jax.ShapeDtypeStruct((bins, k), F32)),
        in_specs=[pl.BlockSpec(memory_space=pltpu.SMEM)] + [whole] * 3,
        out_specs=(whole, whole),
        scratch_shapes=[
            VMEM((steps, TRACK_LEN, k), BF16),
            VMEM((bins, k), F32),
            VMEM((TRACK_LEN, k), F32),
            VMEM((2 * k, 2 * k), F32),
            VMEM((2, 4, block, k), F32),
            VMEM((4, block, k), F32),
            VMEM((half, k), F32),
            VMEM((15, count, k), F32),
            VMEM((15, count, k), F32),
            one((4,)), one((4,)), one, one, one, one, one, one, one, one, one, one,
        ],
        compiler_params=pltpu.CompilerParams(
            collective_id=1 + len(SIZES) + index, has_side_effects=True, vmem_limit_bytes=8 * MIB
        ),
        name=f"templates_{index}",
    )(lengths, act, spectrum, templates)


def store_kernel(placed_ref, out_hbm, sem):
    k = placed_ref.shape[0]
    parts = 8
    copies = []
    for i in range(parts):
        rows = pl.ds(i * (k // parts), k // parts)
        copies.append(pltpu.make_async_copy(placed_ref.at[rows], out_hbm.at[rows], sem.at[i]))
    for copy in copies:
        copy.start()
    for copy in copies:
        copy.wait()


def store_call(placed):
    return pl.pallas_call(
        store_kernel,
        out_shape=jax.ShapeDtypeStruct(placed.shape, placed.dtype),
        in_specs=[pl.BlockSpec(memory_space=VMEM)],
        out_specs=pl.BlockSpec(memory_space=pltpu.HBM),
        scratch_shapes=[pltpu.SemaphoreType.DMA((8,))],
        compiler_params=pltpu.CompilerParams(vmem_limit_bytes=5 * MIB),
        name="store",
    )(placed)


def rest(size, index, src, num, act, operand, lengths, spectrum, templates):
    current = refine_call(size, index, src, num, act, operand)
    current = current.reshape(current.shape[0] // 8, 8, -1)
    placed, new_templates = template_call(index, lengths, current, spectrum, templates)
    return store_call(placed), new_templates


def body(mesh, spectrum, templates, activations, lengths):
    num, act, operand, src, branch, near_spectrum = numerator_call(mesh, spectrum, templates, activations, lengths)
    branches = [functools.partial(rest, size, i) for i, size in enumerate(SIZES)]
    return lax.switch(branch[0], branches, src, num, act, operand, lengths, near_spectrum, templates)


def solution(mesh):
    return jax.shard_map(
        functools.partial(body, mesh),
        mesh=mesh,
        in_specs=(P("freq", "tm"), P("freq", None), P(None, "tm"), P("tm")),
        out_specs=(P(None, "tm"), P("freq", None)),
        check_vma=False,
    )
```
